256 devices in a mesh: dp: 128 (over y, z_hi, x, core), seq: 2 (over z_lo).
Axes of the slice: x: 4, y: 4, z: 8 (z_hi: 4, z_lo: 2; z = z_hi * 2 + z_lo), core: 2. Of those that a mesh axis runs over, the one named last changes fastest.
Arguments:
- activations: bfloat16 [32768, 8192], P(('dp', 'seq')), may hold values from -24 to 24
- queries: bfloat16 [32768, 8192], P(('dp', 'seq')), may hold values from -180 to 180
- keys: bfloat16 [32768, 1024], P(('dp', 'seq')), may hold values from -6 to 6
- out_grad: bfloat16 [32768, 8192], P(('dp', 'seq')), may hold values from -0.03125 to 0.03125
- layout: int32 [8192], replicated, may hold values from 0 to 8191, each once
Outputs:
- value_weight_grad: float32 [8192, 1024], P(('dp', 'seq'))
The draws below stay inside these ranges and needn't reach their ends.
Inputs may be any that keep to these rules, and one draw needn't show every extreme that they name: `layout`: every row number 0 to 8191 appears exactly once.
All inputs are finite; a program needn't handle non-finite values.
Results may differ from the reference program's by a relative error of at most 0.0049.
Values may be sent and summed in bfloat16 or wider, within the bound.
No kernel may reach another device: no remote copies, remote signals or barrier semaphores. Data moves between devices by JAX's collectives and lax.ppermute only.
A program may use at most 128 MiB of HBM per device.

```python
import jax
import jax.numpy as jnp
from jax import lax

D = 8192
H = 64
KVH = 8
HD = 128
LENGTH = 256
TOKENS = 32768


def draw_pair(key):
    base_keys = jnp.clip(jax.random.normal(jax.random.fold_in(key, 11), (TOKENS, KVH * HD), jnp.float32), -6.0, 6.0)
    fresh = jnp.clip(jax.random.normal(jax.random.fold_in(key, 12), (TOKENS, H * HD), jnp.float32), -6.0, 6.0)
    return (fresh, base_keys)


def draw_queries(key, part):
    return draw_pair(key)[0].astype(jnp.bfloat16)


def draw_keys(key, part):
    return draw_pair(key)[1].astype(jnp.bfloat16)


def raised(result, own_key, source, target, blocks, factor):
    owner, partner = [(jnp.arange(result.shape[position]) // (result.shape[position] // blocks)).reshape([-1 if axis == position else 1 for axis in range(result.ndim)]) for position in (source, target)]
    chosen = jax.random.permutation(own_key, blocks)[partner]
    strong = (owner == chosen) | (owner == (partner + blocks // 2) % blocks)
    return jnp.where(strong, factor * result, result)


def block_scale(own_key, dims, split, smallest, high):
    gain, own = 1.0, jax.random.fold_in(own_key, 6)
    for dim, parts in split:
        draws = jnp.exp(jax.random.uniform(jax.random.fold_in(own, dim), (parts,), jnp.float32, smallest / len(split), high / len(split)))
        gain = gain * jnp.repeat(draws, dims[dim] // parts).reshape([-1 if axis == dim else 1 for axis in range(len(dims))])
    return gain


def bell_draw(own_key, extent, spread, limit, shards=(), kind=jnp.bfloat16):
    drawn = spread * jax.random.normal(own_key, extent, jnp.float32)
    if shards:
        drawn = drawn * block_scale(own_key, extent, shards, -0.22, 0.18)
    return jnp.clip(drawn, -limit, limit).astype(kind)


def gaussian_with(rng, extent, width, reach, cuts, heavy, held_as=jnp.bfloat16):
    array = width * jax.random.normal(rng, extent, jnp.float32)
    if cuts:
        array = array * block_scale(rng, extent, cuts, -0.22, 0.18)
    return jnp.clip(raised(array, jax.random.fold_in(rng, 3), *heavy), -reach, reach).astype(held_as)


def setup_inputs(seed: int = 0) -> dict:
    streams_of = jax.random.split(jax.random.key(seed), 6)
    activations = gaussian_with(streams_of[0], (TOKENS, D), 1.0, 24.0, ((0, 256),), (0, 1, 256, 6.0))
    queries = draw_queries(jax.random.fold_in(streams_of[5], 71), 0)
    keys = draw_keys(jax.random.fold_in(streams_of[5], 71), 0)
    out_grad = bell_draw(streams_of[3], (TOKENS, H * HD), ((8 * TOKENS) ** -0.5), 0.03125, ((0, 256),))
    layout = jax.random.permutation(streams_of[4], D).astype(jnp.int32)
    return {"activations": activations, "queries": queries, "keys": keys, "out_grad": out_grad, "layout": layout}


def value_grads(seq_queries, seq_keys, seq_grads):
    length = seq_queries.shape[0]
    per_group = H // KVH
    inv_root = 1.0 / float(HD) ** 0.5
    places = jnp.arange(length)
    allowed = places[:, None] >= places[None, :]
    pieces = []
    for group_index in range(KVH):
        offset = group_index * per_group * HD
        query_block = seq_queries[:, offset:offset + per_group * HD].reshape(length, per_group, HD).astype(jnp.float32)
        grad_block = seq_grads[:, offset:offset + per_group * HD].reshape(length, per_group, HD).astype(jnp.float32)
        key_block = seq_keys[:, group_index * HD:(group_index + 1) * HD].astype(jnp.float32)
        scores = jnp.einsum("igd,jd->gij", query_block, key_block) * inv_root
        scores = jnp.where(allowed[None], scores, -jnp.inf)
        weights = lax.optimization_barrier(jax.nn.softmax(scores, axis=-1).astype(jnp.bfloat16))
        pieces.append(jnp.einsum("gij,igd->jd", weights.astype(jnp.float32), grad_block))
    return jnp.concatenate(pieces, axis=1)


def reference(activations, queries, keys, out_grad, layout):
    count_seqs = activations.shape[0] // LENGTH

    def add_sequence(seq_number, grand_sum):
        first_row = (seq_number * LENGTH).astype(jnp.int32)
        seq_rows = lax.dynamic_slice_in_dim(activations, first_row, LENGTH, 0)
        seq_queries = lax.dynamic_slice_in_dim(queries, first_row, LENGTH, 0)
        seq_keys = lax.dynamic_slice_in_dim(keys, first_row, LENGTH, 0)
        seq_grads = lax.dynamic_slice_in_dim(out_grad, first_row, LENGTH, 0)
        value_grad = value_grads(seq_queries, seq_keys, seq_grads).astype(jnp.bfloat16)
        columns = jnp.take(seq_rows, layout.astype(jnp.int32), axis=1)
        row_term = jnp.dot(columns.T, value_grad, preferred_element_type=jnp.float32)
        row_term = lax.optimization_barrier(row_term.astype(jnp.bfloat16))
        return grand_sum + row_term.astype(jnp.float32)

    return lax.fori_loop(0, count_seqs, add_sequence, jnp.zeros((D, KVH * HD), jnp.float32))
```

```python
import jax
import jax.numpy as jnp
from jax import lax
from jax.experimental import pallas as pl
from jax.experimental.pallas import tpu as pltpu
from jax.sharding import Mesh
from jax.sharding import PartitionSpec as P


H = 64
KVH = 8
HD = 128
PER = H // KVH
AXES = ("y", "zh", "x", "c", "zl")
NEAR = ("x", "c")
CHIPS = 4
OWNED = 32
SCALE = 1.4426950408889634 / float(HD) ** 0.5


def gather_kernel(layout_ref, acts_ref, out_ref, flipped, picked):
    width = acts_ref.shape[1]

    def flip(tile, carry):
        at = pl.multiple_of(tile * 128, 128)
        flipped[pl.ds(at, 128), :] = acts_ref[:, pl.ds(at, 128)].astype(jnp.float32).T
        return carry

    lax.fori_loop(0, width // 128, flip, 0)
    blocks = width // OWNED
    far = out_ref.shape[1] // OWNED
    near = blocks // far

    def pick(block, carry):
        member, owner = block // far, block % far
        base = ((owner // 2 * near + member) * 2 + owner % 2) * OWNED
        for row in range(OWNED):
            source = layout_ref[base + row]
            picked[row : row + 1, :] = flipped[pl.ds(source, 1), :]
        out_ref[member, pl.ds(pl.multiple_of(owner * OWNED, OWNED), OWNED), :] = picked[...].astype(
            jnp.bfloat16
        )
        return carry

    lax.fori_loop(0, blocks, pick, 0)


def gathered(activations, layout, near):
    rows, width = activations.shape
    return pl.pallas_call(
        gather_kernel,
        name="gather_rows",
        out_shape=jax.ShapeDtypeStruct((near, width // near, rows), jnp.bfloat16),
        in_specs=[pl.BlockSpec(memory_space=pltpu.SMEM), pl.BlockSpec(memory_space=pltpu.VMEM)],
        out_specs=pl.BlockSpec(memory_space=pltpu.VMEM),
        scratch_shapes=[
            pltpu.VMEM((width, rows), jnp.float32),
            pltpu.VMEM((OWNED, rows), jnp.float32),
        ],
        cost_estimate=pl.CostEstimate(flops=10**9, bytes_accessed=4 * 2**20, transcendentals=0),
        compiler_params=pltpu.CompilerParams(vmem_limit_bytes=24 * 2**20),
    )(layout, activations)


def attend_kernel(second_ref, queries_ref, earlier_ref, keys_ref, grads_ref, early_ref, own_ref):
    rows = queries_ref.shape[0]
    second = second_ref[0] > 0
    both = jnp.concatenate([earlier_ref[...], keys_ref[...]], axis=0)
    key_place = lax.broadcasted_iota(jnp.int32, (rows, 2 * rows), 0)
    query_place = lax.broadcasted_iota(jnp.int32, (rows, 2 * rows), 1) % rows
    causal = key_place <= query_place
    total = jnp.zeros((2 * rows, HD), jnp.float32)
    for pair in range(PER // 2):
        a, b = 2 * pair * HD, (2 * pair + 1) * HD
        ask = jnp.concatenate([queries_ref[:, a : a + HD], queries_ref[:, b : b + HD]], axis=0)
        grad = jnp.concatenate([grads_ref[:, a : a + HD], grads_ref[:, b : b + HD]], axis=0)
        scores = lax.dot_general(
            both, ask, (((1,), (1,)), ((), ())), preferred_element_type=jnp.float32
        )
        first = jnp.where(second, scores[:rows], -1e30)
        last = jnp.where(causal, scores[rows:], -1e30)
        top = jnp.maximum(
            jnp.max(first, axis=0, keepdims=True), jnp.max(last, axis=0, keepdims=True)
        )
        first = jnp.exp2((first - top) * SCALE)
        last = jnp.exp2((last - top) * SCALE)
        share = 1.0 / (
            jnp.sum(first, axis=0, keepdims=True) + jnp.sum(last, axis=0, keepdims=True)
        )
        weights = jnp.concatenate(
            [(first * share).astype(jnp.bfloat16), (last * share).astype(jnp.bfloat16)], axis=0
        )
        total += jnp.dot(weights, grad, preferred_element_type=jnp.float32)
    early_ref[...] = total[:rows].astype(early_ref.dtype)
    own_ref[...] = total[rows:]


def attended(second, queries, earlier, keys, out_grad):
    rows = queries.shape[0]
    wide = pl.BlockSpec((rows, PER * HD), lambda g: (0, g))
    narrow = pl.BlockSpec((rows, HD), lambda g: (0, g))
    return pl.pallas_call(
        attend_kernel,
        name="attend",
        grid=(KVH,),
        out_shape=(
            jax.ShapeDtypeStruct((rows, KVH * HD), jnp.bfloat16),
            jax.ShapeDtypeStruct((rows, KVH * HD), jnp.float32),
        ),
        in_specs=[pl.BlockSpec(memory_space=pltpu.SMEM), wide, narrow, narrow, wide],
        out_specs=(narrow, narrow),
        cost_estimate=pl.CostEstimate(
            flops=4 * H * rows * 2 * rows * HD,
            bytes_accessed=6 * 2**20,
            transcendentals=H * rows * 2 * rows,
        ),
        compiler_params=pltpu.CompilerParams(vmem_limit_bytes=16 * 2**20),
    )(second, queries, earlier, keys, out_grad)


def multiply_kernel(place_ref, columns_ref, *refs):
    grads, out_ref = refs[:-1], refs[-1]
    chip, core = place_ref[0], place_ref[1]
    tile = 128

    def step(number, carry):
        at = pl.ds(pl.multiple_of(number * tile, tile), tile)
        total = None
        for side in range(2):
            for back in range(0, CHIPS, 2):
                left = jnp.concatenate(
                    [
                        columns_ref[lax.rem(chip + CHIPS - back - more, CHIPS), lax.rem(core + side, 2), at, :]
                        for more in range(2)
                    ],
                    axis=1,
                )
                right = jnp.concatenate(
                    [grads[side * CHIPS + back + more][...] for more in range(2)], axis=0
                )
                term = jnp.dot(left, right, preferred_element_type=jnp.float32)
                total = term if total is None else total + term
        out_ref[at, :] = total.astype(out_ref.dtype)
        return carry

    lax.fori_loop(0, out_ref.shape[0] // tile, step, 0)


def multiplied(where, columns, grads):
    rows, width = columns.shape[2], grads[0].shape[1]
    whole = pl.BlockSpec(memory_space=pltpu.VMEM)
    return pl.pallas_call(
        multiply_kernel,
        name="multiply",
        out_shape=jax.ShapeDtypeStruct((rows, width), jnp.bfloat16),
        in_specs=[pl.BlockSpec(memory_space=pltpu.SMEM)] + [whole] * (1 + len(grads)),
        out_specs=whole,
        cost_estimate=pl.CostEstimate(
            flops=2 * rows * len(grads) * grads[0].shape[0] * width,
            bytes_accessed=8 * 2**20,
            transcendentals=0,
        ),
        compiler_params=pltpu.CompilerParams(vmem_limit_bytes=24 * 2**20),
    )(where, columns, *grads)


def place(axis):
    return lax.axis_index(axis).astype(jnp.int32).reshape(1)


def body(activations, queries, keys, out_grad, layout):
    near = lax.axis_size(NEAR)
    earlier = lax.ppermute(keys, "zl", [(0, 1)])
    columns = gathered(activations, layout, near)
    columns = lax.all_to_all(columns, NEAR, 0, 0, tiled=True)
    early, own = attended(place("zl"), queries, earlier, keys, out_grad)
    returned = lax.ppermute(early, "zl", [(1, 0)])
    value_grad = (own + returned.astype(jnp.float32)).astype(jnp.bfloat16)
    mine = [value_grad] + [
        lax.ppermute(value_grad, "x", [(i, (i + ahead) % CHIPS) for i in range(CHIPS)])
        for ahead in range(1, CHIPS)
    ]
    other = [lax.ppermute(part, "c", [(0, 1), (1, 0)]) for part in mine]
    term = multiplied(
        jnp.concatenate([place("x"), place("c")]),
        columns.reshape(CHIPS, 2, *columns.shape[1:]),
        mine + other,
    )
    width = KVH * HD
    parts = lax.all_to_all(term.reshape(lax.axis_size("y"), -1, width), "y", 0, 0, tiled=True)
    half = jnp.sum(parts.astype(jnp.float32), axis=0).astype(jnp.bfloat16)
    parts = lax.all_to_all(half.reshape(-1, OWNED, width), ("zh", "zl"), 0, 0, tiled=True)
    return jnp.sum(parts.astype(jnp.float32), axis=0)


def solution(mesh):
    finer = Mesh(mesh.devices.reshape(4, 4, 4, 2, mesh.shape["seq"]), AXES)
    placed = (P(AXES, None), P(AXES, None), P(AXES, None), P(AXES, None), P())
    return jax.shard_map(
        body, mesh=finer, in_specs=placed, out_specs=P(AXES, None), check_vma=False
    )
```

```python
import functools

import jax
import jax.numpy as jnp
from jax import lax
from jax.experimental import pallas as pl
from jax.experimental.pallas import tpu as pltpu
from jax.sharding import Mesh
from jax.sharding import PartitionSpec as P


H = 64
KVH = 8
HD = 128
WIDTH = KVH * HD
PER = H // KVH
AXES = ("y", "zh", "x", "c", "zl")
Z = ("zh", "zl")
SIDE, Z_SIZE = 4, 8
OWNED = 32
PART = OWNED // 2
SCALE = 1.4426950408889634 / float(HD) ** 0.5
SMEM = pl.BlockSpec(memory_space=pltpu.SMEM)
VMEM = pl.BlockSpec(memory_space=pltpu.VMEM)


def flip(acts_ref, flipped, landed, arrivals):
    width = acts_ref.shape[1]
    count = arrivals.shape[0]
    share = width // count

    def arriving(part):
        at = pl.ds(pl.multiple_of(part * share, share), share)
        return pltpu.make_async_copy(acts_ref.at[:, at], landed.at[:, at], arrivals.at[part])

    for part in range(count):
        arriving(part).start()

    def step(part, carry):
        arriving(part).wait()
        for tile in range(share // 128):
            at = pl.ds(pl.multiple_of(part * share + tile * 128, 128), 128)
            flipped[at, :] = landed[:, at].astype(jnp.float32).T
        return carry

    lax.fori_loop(0, count, step, 0)


def pick(routes, place_ref, layout_ref, flipped, picked, outs):
    y, z, x, core = (place_ref[i] for i in range(4))
    for (axis, steps), out_ref in zip(routes, outs):

        def step(tile, carry):
            to_core, off = (core + (tile >> 2)) & 1, tile & (SIDE - 1)
            x_steps, y_steps = (steps, off) if axis == "x" else (off, steps)
            to_x, to_y = (x + x_steps) & (SIDE - 1), (y + y_steps) & (SIDE - 1)
            for block in range(Z_SIZE):
                to_z = (z + block) & (Z_SIZE - 1)
                owner = ((((to_y * 4 + (to_z >> 1)) * 4 + to_x) * 2 + to_core) * 2) + (to_z & 1)
                base = owner * OWNED + (0 if axis == "x" else PART)
                for row in range(PART):
                    source = layout_ref[base + row]
                    at = block * PART + row
                    picked[at : at + 1, :] = flipped[pl.ds(source, 1), :]
            rows = Z_SIZE * PART
            out_ref[pl.ds(pl.multiple_of(tile * rows, rows), rows), :] = picked[...].astype(
                jnp.bfloat16
            )
            return carry

        lax.fori_loop(0, 2 * SIDE, step, 0)


def first_pick_kernel(routes, place_ref, layout_ref, acts_ref, flipped, *refs):
    outs = refs[: len(routes)]
    picked, landed, arrivals, rows_ref, rows_arrival = refs[len(routes) :]
    rows_copy = pltpu.make_async_copy(layout_ref, rows_ref, rows_arrival)
    rows_copy.start()
    flip(acts_ref, flipped, landed, arrivals)
    rows_copy.wait()
    pick(routes, place_ref, rows_ref, flipped, picked, outs)


def later_pick_kernel(routes, place_ref, layout_ref, flipped, *refs):
    pick(routes, place_ref, layout_ref, flipped, refs[-1], refs[:-1])


def picked_rows(routes, where, layout, source, first):
    tokens = 128
    width = layout.shape[0]
    piece = jax.ShapeDtypeStruct((2 * SIDE * Z_SIZE * PART, tokens), jnp.bfloat16)
    shapes = [piece] * len(routes)
    scratch = [pltpu.VMEM((Z_SIZE * PART, tokens), jnp.float32)]
    if first:
        shapes = [jax.ShapeDtypeStruct((width, tokens), jnp.float32)] + shapes
        scratch += [
            pltpu.VMEM((tokens, width), jnp.bfloat16),
            pltpu.SemaphoreType.DMA((8,)),
            pltpu.SMEM((width,), jnp.int32),
            pltpu.SemaphoreType.DMA,
        ]
    far = pl.BlockSpec(memory_space=pl.ANY)
    return pl.pallas_call(
        functools.partial(first_pick_kernel if first else later_pick_kernel, routes),
        name="pick",
        out_shape=tuple(shapes),
        in_specs=[SMEM, far, far] if first else [SMEM, SMEM, VMEM],
        out_specs=tuple([VMEM] * len(shapes)),
        scratch_shapes=scratch,
        cost_estimate=pl.CostEstimate(
            flops=10**9 * len(routes), bytes_accessed=4 * 2**20, transcendentals=0
        ),
        compiler_params=pltpu.CompilerParams(vmem_limit_bytes=16 * 2**20),
    )(where, layout, source)


def attend_kernel(
    first, groups, place_ref, queries_ref, earlier_ref, keys_ref, grads_ref, early_ref, own_ref
):
    rows = queries_ref.shape[0]
    second = (place_ref[1] & 1) > 0
    shape = (rows, rows)
    causal = lax.broadcasted_iota(jnp.int32, shape, 0) <= lax.broadcasted_iota(jnp.int32, shape, 1)

    def group(number, carry):
        head = pl.ds(pl.multiple_of((number + first) * HD, HD), HD)
        both = jnp.concatenate([earlier_ref[:, head], keys_ref[:, head]], axis=0)
        total = jnp.zeros((2 * rows, HD), jnp.float32)
        for query_head in range(PER):
            at = pl.ds(pl.multiple_of(((number + first) * PER + query_head) * HD, HD), HD)
            scores = lax.dot_general(
                both, queries_ref[:, at], (((1,), (1,)), ((), ())), preferred_element_type=jnp.float32
            )
            before = jnp.where(second, scores[:rows], -1e30)
            last = jnp.where(causal, scores[rows:], -1e30)
            top = jnp.maximum(
                jnp.max(before, axis=0, keepdims=True), jnp.max(last, axis=0, keepdims=True)
            )
            before = jnp.exp2((before - top) * SCALE)
            last = jnp.exp2((last - top) * SCALE)
            share = 1.0 / (
                jnp.sum(before, axis=0, keepdims=True) + jnp.sum(last, axis=0, keepdims=True)
            )
            weights = jnp.concatenate(
                [(before * share).astype(jnp.bfloat16), (last * share).astype(jnp.bfloat16)], axis=0
            )
            total += jnp.dot(weights, grads_ref[:, at], preferred_element_type=jnp.float32)
        out = pl.ds(pl.multiple_of(number * HD, HD), HD)
        early_ref[:, out] = total[:rows].astype(early_ref.dtype)
        own_ref[:, out] = total[rows:]
        return carry

    lax.fori_loop(0, groups, group, 0)


def attended(first, groups, where, queries, earlier, keys, out_grad):
    rows = queries.shape[0]
    return pl.pallas_call(
        functools.partial(attend_kernel, first, groups),
        name="attend",
        out_shape=(
            jax.ShapeDtypeStruct((rows, groups * HD), jnp.bfloat16),
            jax.ShapeDtypeStruct((rows, groups * HD), jnp.float32),
        ),
        in_specs=[SMEM, VMEM, VMEM, VMEM, VMEM],
        out_specs=(VMEM, VMEM),
        cost_estimate=pl.CostEstimate(
            flops=4 * groups * PER * rows * 2 * rows * HD,
            bytes_accessed=3 * 2**20,
            transcendentals=groups * PER * rows * 2 * rows,
        ),
        compiler_params=pltpu.CompilerParams(vmem_limit_bytes=16 * 2**20),
    )(where, queries, earlier, keys, out_grad)


def multiply_kernel(*refs):
    columns, grads, (own_ref, away_ref) = refs[:SIDE], refs[SIDE : 2 * SIDE], refs[2 * SIDE :]
    tile = 256
    half = own_ref.shape[0]
    for number in range(2 * half // tile):
        at = slice(number * tile, (number + 1) * tile)
        total = None
        for i in range(0, SIDE, 2):
            left = jnp.concatenate([columns[i][at, :], columns[i + 1][at, :]], axis=1)
            right = jnp.concatenate([grads[i][...], grads[i + 1][...]], axis=0)
            term = jnp.dot(left, right, preferred_element_type=jnp.float32)
            total = term if total is None else total + term
        if number * tile < half:
            own_ref[at, :] = total
        else:
            away_ref[number * tile - half : (number + 1) * tile - half, :] = total.astype(
                away_ref.dtype
            )


def multiplied(columns, grads):
    half = columns[0].shape[0] // 2
    return pl.pallas_call(
        multiply_kernel,
        name="multiply",
        out_shape=(
            jax.ShapeDtypeStruct((half, WIDTH), jnp.float32),
            jax.ShapeDtypeStruct((half, WIDTH), jnp.bfloat16),
        ),
        in_specs=[VMEM] * (2 * SIDE),
        out_specs=(VMEM, VMEM),
        cost_estimate=pl.CostEstimate(
            flops=4 * half * SIDE * 128 * WIDTH, bytes_accessed=4 * 2**20, transcendentals=0
        ),
        compiler_params=pltpu.CompilerParams(vmem_limit_bytes=16 * 2**20),
    )(*columns, *grads)


def merge_kernel(own_ref, got_ref, *outs):
    rows = outs[0].shape[0]
    for number, out_ref in enumerate(outs):
        at = slice(number * rows, (number + 1) * rows)
        out_ref[...] = (own_ref[at, :] + got_ref[at, :].astype(jnp.float32)).astype(out_ref.dtype)


def merged(own, got):
    shape = jax.ShapeDtypeStruct((own.shape[0] // SIDE, WIDTH), jnp.bfloat16)
    return pl.pallas_call(
        merge_kernel,
        name="merge",
        out_shape=tuple([shape] * SIDE),
        in_specs=[VMEM, VMEM],
        out_specs=tuple([VMEM] * SIDE),
        cost_estimate=pl.CostEstimate(flops=5 * 10**8, bytes_accessed=2**20, transcendentals=0),
        compiler_params=pltpu.CompilerParams(vmem_limit_bytes=4 * 2**20),
    )(own, got)


def halfway_kernel(place_ref, *refs):
    out_ref = refs[-1]
    z = place_ref[1]
    for way in range(2):
        parts = refs[way * SIDE : (way + 1) * SIDE]
        for block in range(Z_SIZE):
            at = slice(block * PART, (block + 1) * PART)
            total = parts[0][at, :].astype(jnp.float32)
            for part in parts[1:]:
                total += part[at, :].astype(jnp.float32)
            out_ref[(z + block) & (Z_SIZE - 1), way * PART : (way + 1) * PART, :] = total.astype(
                out_ref.dtype
            )


def halfway(where, parts):
    return pl.pallas_call(
        halfway_kernel,
        name="halfway",
        out_shape=jax.ShapeDtypeStruct((Z_SIZE, OWNED, WIDTH), jnp.bfloat16),
        in_specs=[SMEM] + [VMEM] * len(parts),
        out_specs=VMEM,
        cost_estimate=pl.CostEstimate(flops=5 * 10**8, bytes_accessed=2**20, transcendentals=0),
        compiler_params=pltpu.CompilerParams(vmem_limit_bytes=4 * 2**20),
    )(where, *parts)


def finish_kernel(parts_ref, out_ref):
    total = parts_ref[0].astype(jnp.float32)
    for part in range(1, Z_SIZE):
        total += parts_ref[part].astype(jnp.float32)
    out_ref[...] = total


def finished(parts):
    return pl.pallas_call(
        finish_kernel,
        name="finish",
        out_shape=jax.ShapeDtypeStruct((OWNED, WIDTH), jnp.float32),
        in_specs=[VMEM],
        out_specs=VMEM,
        cost_estimate=pl.CostEstimate(flops=5 * 10**8, bytes_accessed=2**20, transcendentals=0),
        compiler_params=pltpu.CompilerParams(vmem_limit_bytes=4 * 2**20),
    )(parts)


def ahead(value, axis, steps):
    count = lax.axis_size(axis)
    return lax.ppermute(value, axis, [(i, (i + steps) % count) for i in range(count)])


FAR = (("x", 2), ("y", 2))
NEXT = (("x", 1), ("x", 3), ("y", 1), ("y", 3))
HERE = (("x", 0), ("y", 0))


def body(activations, queries, keys, out_grad, layout):
    where = jnp.stack([lax.axis_index(axis).astype(jnp.int32) for axis in ("y", Z, "x", "c")])
    columns = {}
    earlier = lax.ppermute(keys, "zl", [(0, 1)])
    flipped, *pieces = picked_rows(FAR, where, layout, activations, True)
    for route, piece in zip(FAR, pieces):
        columns[route] = ahead(piece, *route)
    groups = KVH // 2
    own, returned = [], []
    for half in range(2):
        early, mine = attended(half * groups, groups, where, queries, earlier, keys, out_grad)
        own.append(mine)
        returned.append(lax.ppermute(early, "zl", [(1, 0)]))
    pieces = picked_rows(NEXT, where, layout, flipped, False)
    for route, piece in zip(NEXT, pieces):
        columns[route] = ahead(piece, *route)
    pieces = picked_rows(HERE, where, layout, flipped, False)
    columns.update(zip(HERE, pieces))
    value_grad = jnp.concatenate(
        [(a + b.astype(jnp.float32)).astype(jnp.bfloat16) for a, b in zip(own, returned)], axis=1
    )
    grads = {route: value_grad for route in HERE}
    for route in FAR + NEXT:
        grads[route] = ahead(value_grad, *route)
    parts = []
    for way, across in (("x", "y"), ("y", "x")):
        routes = [(way, steps) for steps in range(SIDE)]
        kept, away = multiplied([columns[r] for r in routes], [grads[r] for r in routes])
        got = ahead(away, "c", 1)
        terms = merged(kept, got)
        parts += [terms[0]] + [ahead(terms[i], across, i) for i in range(1, SIDE)]
    terms = halfway(where, parts)
    terms = lax.all_to_all(terms, Z, 0, 0, tiled=True)
    return finished(terms)


def solution(mesh):
    finer = Mesh(mesh.devices.reshape(4, 4, 4, 2, mesh.shape["seq"]), AXES)
    placed = (P(AXES, None), P(AXES, None), P(AXES, None), P(AXES, None), P())
    return jax.shard_map(
        body, mesh=finer, in_specs=placed, out_specs=P(AXES, None), check_vma=False
    )
```

```python
import functools

import jax
import jax.numpy as jnp
from jax import lax
from jax.experimental import pallas as pl
from jax.experimental.pallas import tpu as pltpu
from jax.sharding import Mesh
from jax.sharding import PartitionSpec as P


H = 64
KVH = 8
HD = 128
WIDTH = KVH * HD
PER = H // KVH
AXES = ("y", "zh", "x", "c", "zl")
Z = ("zh", "zl")
SIDE, Z_SIZE = 4, 8
OWNED = 32
PART = OWNED // 2
COLUMNS = 2 * SIDE * Z_SIZE * PART
SCALE = 1.4426950408889634 / float(HD) ** 0.5
SMEM = pl.BlockSpec(memory_space=pltpu.SMEM)
VMEM = pl.BlockSpec(memory_space=pltpu.VMEM)


def flip(acts_ref, flipped, landed, arrivals):
    width = acts_ref.shape[1]
    count = arrivals.shape[0]
    share = width // count

    def arriving(part):
        at = pl.ds(pl.multiple_of(part * share, share), share)
        return pltpu.make_async_copy(acts_ref.at[:, at], landed.at[:, at], arrivals.at[part])

    for part in range(count):
        arriving(part).start()

    def step(part, carry):
        arriving(part).wait()
        for tile in range(share // 128):
            at = pl.ds(pl.multiple_of(part * share + tile * 128, 128), 128)
            flipped[at, :] = landed[:, at].astype(jnp.float32).T
        return carry

    lax.fori_loop(0, count, step, 0)


def pick(routes, place_ref, layout_ref, flipped, picked, outs):
    y, z, x, core = (place_ref[i] for i in range(4))
    for (axis, steps), out_ref in zip(routes, outs):

        def step(tile, carry):
            to_core, off = (core + (tile >> 2)) & 1, tile & (SIDE - 1)
            x_steps, y_steps = (steps, off) if axis == "x" else (off, steps)
            to_x, to_y = (x + x_steps) & (SIDE - 1), (y + y_steps) & (SIDE - 1)
            for block in range(Z_SIZE):
                to_z = (z + block) & (Z_SIZE - 1)
                owner = ((((to_y * 4 + (to_z >> 1)) * 4 + to_x) * 2 + to_core) * 2) + (to_z & 1)
                base = owner * OWNED + (0 if axis == "x" else PART)
                for row in range(PART):
                    source = layout_ref[base + row]
                    at = block * PART + row
                    picked[at : at + 1, :] = flipped[pl.ds(source, 1), :]
            rows = Z_SIZE * PART
            out_ref[pl.ds(pl.multiple_of(tile * rows, rows), rows), :] = picked[...].astype(
                jnp.bfloat16
            )
            return carry

        lax.fori_loop(0, 2 * SIDE, step, 0)


def first_pick_kernel(routes, place_ref, layout_ref, acts_ref, flipped, *refs):
    outs = refs[: len(routes)]
    picked, landed, arrivals, rows_ref, rows_arrival = refs[len(routes) :]
    rows_copy = pltpu.make_async_copy(layout_ref, rows_ref, rows_arrival)
    rows_copy.start()
    flip(acts_ref, flipped, landed, arrivals)
    rows_copy.wait()
    pick(routes, place_ref, rows_ref, flipped, picked, outs)


def later_pick_kernel(routes, place_ref, layout_ref, flipped, *refs):
    pick(routes, place_ref, layout_ref, flipped, refs[-1], refs[:-1])


def picked_rows(routes, where, layout, source, first, spare=0):
    tokens = 128
    width = layout.shape[0]
    piece = jax.ShapeDtypeStruct((COLUMNS + spare, tokens), jnp.bfloat16)
    shapes = [piece] * len(routes)
    scratch = [pltpu.VMEM((Z_SIZE * PART, tokens), jnp.float32)]
    if first:
        shapes = [jax.ShapeDtypeStruct((width, tokens), jnp.float32)] + shapes
        scratch += [
            pltpu.VMEM((tokens, width), jnp.bfloat16),
            pltpu.SemaphoreType.DMA((8,)),
            pltpu.SMEM((width,), jnp.int32),
            pltpu.SemaphoreType.DMA,
        ]
    far = pl.BlockSpec(memory_space=pltpu.HBM)
    return pl.pallas_call(
        functools.partial(first_pick_kernel if first else later_pick_kernel, routes),
        name="pick",
        out_shape=tuple(shapes),
        in_specs=[SMEM, far, far] if first else [SMEM, SMEM, VMEM],
        out_specs=tuple([VMEM] * len(shapes)),
        scratch_shapes=scratch,
        cost_estimate=pl.CostEstimate(
            flops=10**9 * len(routes), bytes_accessed=4 * 2**20, transcendentals=0
        ),
        compiler_params=pltpu.CompilerParams(vmem_limit_bytes=16 * 2**20),
    )(where, layout, source)


def attend_kernel(
    first, groups, place_ref, queries_ref, earlier_ref, keys_ref, grads_ref, early_ref, own_ref
):
    rows = queries_ref.shape[0]
    second = (place_ref[1] & 1) > 0
    shape = (rows, rows)
    causal = lax.broadcasted_iota(jnp.int32, shape, 0) <= lax.broadcasted_iota(jnp.int32, shape, 1)

    def group(number, carry):
        head = pl.ds(pl.multiple_of((number + first) * HD, HD), HD)
        both = jnp.concatenate([earlier_ref[:, head], keys_ref[:, head]], axis=0)
        total = jnp.zeros((2 * rows, HD), jnp.float32)
        for query_head in range(PER):
            at = pl.ds(pl.multiple_of(((number + first) * PER + query_head) * HD, HD), HD)
            scores = lax.dot_general(
                both, queries_ref[:, at], (((1,), (1,)), ((), ())), preferred_element_type=jnp.float32
            )
            before = jnp.where(second, scores[:rows], -1e30)
            last = jnp.where(causal, scores[rows:], -1e30)
            top = jnp.maximum(
                jnp.max(before, axis=0, keepdims=True), jnp.max(last, axis=0, keepdims=True)
            )
            before = jnp.exp2((before - top) * SCALE)
            last = jnp.exp2((last - top) * SCALE)
            share = 1.0 / (
                jnp.sum(before, axis=0, keepdims=True) + jnp.sum(last, axis=0, keepdims=True)
            )
            weights = jnp.concatenate(
                [(before * share).astype(jnp.bfloat16), (last * share).astype(jnp.bfloat16)], axis=0
            )
            total += jnp.dot(weights, grads_ref[:, at], preferred_element_type=jnp.float32)
        out = pl.ds(pl.multiple_of(number * HD, HD), HD)
        early_ref[:, out] = total[:rows].astype(early_ref.dtype)
        own_ref[:, out] = total[rows:]
        return carry

    lax.fori_loop(0, groups, group, 0)


def attended(first, groups, where, queries, earlier, keys, out_grad):
    rows = queries.shape[0]
    return pl.pallas_call(
        functools.partial(attend_kernel, first, groups),
        name="attend",
        out_shape=(
            jax.ShapeDtypeStruct((rows, groups * HD), jnp.bfloat16),
            jax.ShapeDtypeStruct((rows, groups * HD), jnp.float32),
        ),
        in_specs=[SMEM, VMEM, VMEM, VMEM, VMEM],
        out_specs=(VMEM, VMEM),
        cost_estimate=pl.CostEstimate(
            flops=4 * groups * PER * rows * 2 * rows * HD,
            bytes_accessed=3 * 2**20,
            transcendentals=groups * PER * rows * 2 * rows,
        ),
        compiler_params=pltpu.CompilerParams(vmem_limit_bytes=16 * 2**20),
    )(where, queries, earlier, keys, out_grad)


def completed_kernel(count, *refs):
    own, returned = refs[:2], refs[2:4]
    grads_ref, *sent = refs[4 + count : 5 + 2 * count]
    tokens = own[0].shape[0]
    for half in range(2):
        for block in range(KVH // 2):
            at = slice(block * HD, (block + 1) * HD)
            row = (half * KVH // 2 + block) * tokens
            grads_ref[row : row + tokens, :] = (
                own[half][:, at] + returned[half][:, at].astype(jnp.float32)
            ).astype(jnp.bfloat16)
    for out_ref in sent:
        out_ref[COLUMNS:, :] = grads_ref[...]


def completed(own, returned, pieces):
    count = len(pieces)
    shape = jax.ShapeDtypeStruct((KVH * own[0].shape[0], HD), jnp.bfloat16)
    return pl.pallas_call(
        functools.partial(completed_kernel, count),
        name="complete",
        out_shape=(shape, *(jax.ShapeDtypeStruct(p.shape, p.dtype) for p in pieces)),
        in_specs=[VMEM] * (4 + count),
        out_specs=tuple([VMEM] * (1 + count)),
        input_output_aliases={4 + i: 1 + i for i in range(count)},
        cost_estimate=pl.CostEstimate(flops=5 * 10**8, bytes_accessed=2**20, transcendentals=0),
        compiler_params=pltpu.CompilerParams(vmem_limit_bytes=4 * 2**20),
    )(*own, *returned, *pieces)


def multiply_kernel(places, away, *refs):
    tile = 256
    first = COLUMNS // 2 if away else 0
    if away:
        arrays, outs = refs[:-1], refs[-1:]
    else:
        arrays, got_ref, outs = refs[: -1 - SIDE], refs[-1 - SIDE], refs[-SIDE:]
    tokens = arrays[0].shape[1]
    rows = outs[0].shape[0]

    def right(place):
        which, base = place
        return jnp.concatenate(
            [
                arrays[which][base + block * tokens : base + (block + 1) * tokens, :]
                for block in range(KVH)
            ],
            axis=1,
        )

    for number in range(COLUMNS // 2 // tile):
        at = slice(first + number * tile, first + (number + 1) * tile)
        total = None
        for i in range(0, SIDE, 2):
            (left_a, grads_a), (left_b, grads_b) = places[i], places[i + 1]
            left = jnp.concatenate([arrays[left_a][at, :], arrays[left_b][at, :]], axis=1)
            both = jnp.concatenate([right(grads_a), right(grads_b)], axis=0)
            term = jnp.dot(left, both, preferred_element_type=jnp.float32)
            total = term if total is None else total + term
        if not away:
            total += got_ref[at, :].astype(jnp.float32)
        total = total.astype(jnp.bfloat16)
        for start in range(number * tile, (number + 1) * tile, min(rows, tile)):
            count = min(rows, tile)
            base = start % rows
            outs[start // rows][base : base + count, :] = total[
                start - number * tile : start - number * tile + count
            ]


def multiplied(pairs, got=None):
    arrays, places = [], []
    for columns, grads in pairs:
        arrays.append(columns)
        left = len(arrays) - 1
        if grads is None:
            places.append((left, (left, COLUMNS)))
        else:
            arrays.append(grads)
            places.append((left, (left + 1, 0)))
    half = COLUMNS // 2
    away = got is None
    count, rows = (1, half) if away else (SIDE, half // SIDE)
    if not away:
        arrays.append(got)
    return pl.pallas_call(
        functools.partial(multiply_kernel, tuple(places), away),
        name="multiply",
        out_shape=tuple([jax.ShapeDtypeStruct((rows, WIDTH), jnp.bfloat16)] * count),
        in_specs=[VMEM] * len(arrays),
        out_specs=tuple([VMEM] * count),
        cost_estimate=pl.CostEstimate(
            flops=2 * half * SIDE * 128 * WIDTH, bytes_accessed=4 * 2**20, transcendentals=0
        ),
        compiler_params=pltpu.CompilerParams(vmem_limit_bytes=16 * 2**20),
    )(*arrays)


def halfway_kernel(place_ref, *refs):
    out_ref = refs[-1]
    z = place_ref[1]
    for way in range(2):
        parts = refs[way * SIDE : (way + 1) * SIDE]
        for block in range(Z_SIZE):
            at = slice(block * PART, (block + 1) * PART)
            total = parts[0][at, :].astype(jnp.float32)
            for part in parts[1:]:
                total += part[at, :].astype(jnp.float32)
            out_ref[(z + block) & (Z_SIZE - 1), way * PART : (way + 1) * PART, :] = total.astype(
                out_ref.dtype
            )


def halfway(where, parts):
    return pl.pallas_call(
        halfway_kernel,
        name="halfway",
        out_shape=jax.ShapeDtypeStruct((Z_SIZE, OWNED, WIDTH), jnp.bfloat16),
        in_specs=[SMEM] + [VMEM] * len(parts),
        out_specs=VMEM,
        cost_estimate=pl.CostEstimate(flops=5 * 10**8, bytes_accessed=2**20, transcendentals=0),
        compiler_params=pltpu.CompilerParams(vmem_limit_bytes=4 * 2**20),
    )(where, *parts)


def finish_kernel(parts_ref, out_ref):
    total = parts_ref[0].astype(jnp.float32)
    for part in range(1, Z_SIZE):
        total += parts_ref[part].astype(jnp.float32)
    out_ref[...] = total


def finished(parts):
    return pl.pallas_call(
        finish_kernel,
        name="finish",
        out_shape=jax.ShapeDtypeStruct((OWNED, WIDTH), jnp.float32),
        in_specs=[VMEM],
        out_specs=VMEM,
        cost_estimate=pl.CostEstimate(flops=5 * 10**8, bytes_accessed=2**20, transcendentals=0),
        compiler_params=pltpu.CompilerParams(vmem_limit_bytes=4 * 2**20),
    )(parts)


def ahead(value, axis, steps):
    count = lax.axis_size(axis)
    return lax.ppermute(value, axis, [(i, (i + steps) % count) for i in range(count)])


FAR = (("x", 2), ("y", 2))
NEXT = (("x", 1), ("x", 3), ("y", 1), ("y", 3))
HERE = (("x", 0), ("y", 0))


def body(activations, queries, keys, out_grad, layout):
    where = jnp.stack([lax.axis_index(axis).astype(jnp.int32) for axis in ("y", Z, "x", "c")])
    columns = {}
    earlier = lax.ppermute(keys, "zl", [(0, 1)])
    flipped, *pieces = picked_rows(
        FAR,
        where,
        pltpu.with_memory_space_constraint(layout, pltpu.HBM),
        pltpu.with_memory_space_constraint(activations, pltpu.HBM),
        True,
    )
    for route, piece in zip(FAR, pieces):
        columns[route] = ahead(piece, *route)
    groups = KVH // 2
    own, returned = [], []
    for half in range(2):
        early, mine = attended(half * groups, groups, where, queries, earlier, keys, out_grad)
        own.append(mine)
        returned.append(lax.ppermute(early, "zl", [(1, 0)]))
    pieces = picked_rows(NEXT, where, layout, flipped, False, WIDTH)
    value_grad, *pieces = completed(own, returned, pieces)
    pairs = {}
    for route, piece in zip(NEXT, pieces):
        pairs[route] = (ahead(piece, *route), None)
    for route in FAR:
        pairs[route] = (columns[route], ahead(value_grad, *route))
    pieces = picked_rows(HERE, where, layout, flipped, False)
    for route, piece in zip(HERE, pieces):
        pairs[route] = (piece, value_grad)
    ways = {way: [pairs[way, steps] for steps in range(SIDE)] for way in ("x", "y")}
    got = {}
    for way in ways:
        (away,) = multiplied(ways[way])
        got[way] = ahead(away, "c", 1)
    parts = []
    for way, across in (("x", "y"), ("y", "x")):
        terms = multiplied(ways[way], got[way])
        moved = [terms[0]]
        for steps in range(1, SIDE):
            moved.append(ahead(terms[steps], across, steps))
        parts += moved
    terms = halfway(where, parts)
    terms = lax.all_to_all(terms, Z, 0, 0, tiled=True)
    return finished(terms)


def solution(mesh):
    finer = Mesh(mesh.devices.reshape(4, 4, 4, 2, mesh.shape["seq"]), AXES)
    placed = (P(AXES, None), P(AXES, None), P(AXES, None), P(AXES, None), P())
    return jax.shard_map(
        body, mesh=finer, in_specs=placed, out_specs=P(AXES, None), check_vma=False
    )
```

```python
import functools

import jax
import jax.numpy as jnp
from jax import lax
from jax.experimental import pallas as pl
from jax.experimental.pallas import tpu as pltpu
from jax.sharding import Mesh
from jax.sharding import PartitionSpec as P


H = 64
KVH = 8
HD = 128
WIDTH = KVH * HD
PER = H // KVH
AXES = ("y", "zh", "x", "c", "zl")
Z = ("zh", "zl")
SIDE, Z_SIZE = 4, 8
OWNED = 32
COLUMNS = SIDE * Z_SIZE * OWNED
WAYS = ("x", "y")
SCALE = 1.4426950408889634 / float(HD) ** 0.5
SMEM = pl.BlockSpec(memory_space=pltpu.SMEM)
VMEM = pl.BlockSpec(memory_space=pltpu.VMEM)


def flip(acts_ref, flipped, landed, arrivals):
    width = acts_ref.shape[1]
    count = arrivals.shape[0]
    share = width // count

    def arriving(part):
        at = pl.ds(pl.multiple_of(part * share, share), share)
        return pltpu.make_async_copy(acts_ref.at[:, at], landed.at[:, at], arrivals.at[part])

    for part in range(count):
        arriving(part).start()

    def step(part, carry):
        arriving(part).wait()
        for tile in range(share // 128):
            at = pl.ds(pl.multiple_of(part * share + tile * 128, 128), 128)
            flipped[at, :] = landed[:, at].astype(jnp.float32).T
        return carry

    lax.fori_loop(0, count, step, 0)


def pick(routes, layout_ref, flipped, picked, outs):
    y, z, x = (lax.axis_index(axis) for axis in ("y", Z, "x"))
    for (axis, steps), out_ref in zip(routes, outs):

        def step(tile, carry):
            off = tile >> 1
            x_steps, y_steps = (steps, off) if axis == "x" else (off, steps)
            to_x, to_y = (x + x_steps) & (SIDE - 1), (y + y_steps) & (SIDE - 1)
            for block in range(Z_SIZE // 2):
                to_z = (z + (tile & 1) * (Z_SIZE // 2) + block) & (Z_SIZE - 1)
                owner = (((to_y * 4 + (to_z >> 1)) * 4 + to_x) * 2 + WAYS.index(axis)) * 2 + (to_z & 1)
                for row in range(OWNED):
                    source = layout_ref[owner * OWNED + row]
                    at = block * OWNED + row
                    picked[at : at + 1, :] = flipped[pl.ds(source, 1), :]
            rows = Z_SIZE // 2 * OWNED
            out_ref[pl.ds(pl.multiple_of(tile * rows, rows), rows), :] = picked[...].astype(
                jnp.bfloat16
            )
            return carry

        lax.fori_loop(0, 2 * SIDE, step, 0)


def first_pick_kernel(routes, layout_ref, acts_ref, flipped, *refs):
    outs = refs[: len(routes)]
    picked, landed, arrivals, rows_ref, rows_arrival = refs[len(routes) :]
    rows_copy = pltpu.make_async_copy(layout_ref, rows_ref, rows_arrival)
    rows_copy.start()
    flip(acts_ref, flipped, landed, arrivals)
    rows_copy.wait()
    pick(routes, rows_ref, flipped, picked, outs)


def later_pick_kernel(routes, layout_ref, flipped, *refs):
    pick(routes, layout_ref, flipped, refs[-1], refs[:-1])


def picked_rows(routes, layout, source, first, spare=0):
    tokens = 128
    width = layout.shape[0]
    piece = jax.ShapeDtypeStruct((COLUMNS + spare, tokens), jnp.bfloat16)
    shapes = [piece] * len(routes)
    scratch = [pltpu.VMEM((Z_SIZE // 2 * OWNED, tokens), jnp.float32)]
    if first:
        shapes = [jax.ShapeDtypeStruct((width, tokens), jnp.float32)] + shapes
        scratch += [
            pltpu.VMEM((tokens, width), jnp.bfloat16),
            pltpu.SemaphoreType.DMA((8,)),
            pltpu.SMEM((width,), jnp.int32),
            pltpu.SemaphoreType.DMA,
        ]
    far = pl.BlockSpec(memory_space=pltpu.HBM)
    return pl.pallas_call(
        functools.partial(first_pick_kernel if first else later_pick_kernel, routes),
        name="pick",
        out_shape=tuple(shapes),
        in_specs=[far, far] if first else [SMEM, VMEM],
        out_specs=tuple([VMEM] * len(shapes)),
        scratch_shapes=scratch,
        cost_estimate=pl.CostEstimate(
            flops=10**9 * len(routes), bytes_accessed=4 * 2**20, transcendentals=0
        ),
        compiler_params=pltpu.CompilerParams(vmem_limit_bytes=16 * 2**20),
    )(layout, source)


def attend_kernel(
    first, groups, queries_ref, earlier_ref, keys_ref, grads_ref, early_ref, own_ref
):
    rows = queries_ref.shape[0]
    second = lax.axis_index("zl") > 0
    shape = (rows, rows)
    causal = lax.broadcasted_iota(jnp.int32, shape, 0) <= lax.broadcasted_iota(jnp.int32, shape, 1)

    def group(number, carry):
        head = pl.ds(pl.multiple_of((number + first) * HD, HD), HD)
        both = jnp.concatenate([earlier_ref[:, head], keys_ref[:, head]], axis=0)
        total = jnp.zeros((2 * rows, HD), jnp.float32)
        for query_head in range(PER):
            at = pl.ds(pl.multiple_of(((number + first) * PER + query_head) * HD, HD), HD)
            scores = lax.dot_general(
                both, queries_ref[:, at], (((1,), (1,)), ((), ())), preferred_element_type=jnp.float32
            )
            before = jnp.where(second, scores[:rows], -1e30)
            last = jnp.where(causal, scores[rows:], -1e30)
            top = jnp.maximum(
                jnp.max(before, axis=0, keepdims=True), jnp.max(last, axis=0, keepdims=True)
            )
            before = jnp.exp2((before - top) * SCALE)
            last = jnp.exp2((last - top) * SCALE)
            share = 1.0 / (
                jnp.sum(before, axis=0, keepdims=True) + jnp.sum(last, axis=0, keepdims=True)
            )
            weights = jnp.concatenate(
                [(before * share).astype(jnp.bfloat16), (last * share).astype(jnp.bfloat16)], axis=0
            )
            total += jnp.dot(weights, grads_ref[:, at], preferred_element_type=jnp.float32)
        out = pl.ds(pl.multiple_of(number * HD, HD), HD)
        early_ref[:, out] = total[:rows].astype(early_ref.dtype)
        own_ref[:, out] = total[rows:]
        return carry

    lax.fori_loop(0, groups, group, 0)


def attended(first, groups, queries, earlier, keys, out_grad):
    rows = queries.shape[0]
    return pl.pallas_call(
        functools.partial(attend_kernel, first, groups),
        name="attend",
        out_shape=(
            jax.ShapeDtypeStruct((rows, groups * HD), jnp.bfloat16),
            jax.ShapeDtypeStruct((rows, groups * HD), jnp.float32),
        ),
        in_specs=[VMEM, VMEM, VMEM, VMEM],
        out_specs=(VMEM, VMEM),
        cost_estimate=pl.CostEstimate(
            flops=4 * groups * PER * rows * 2 * rows * HD,
            bytes_accessed=3 * 2**20,
            transcendentals=groups * PER * rows * 2 * rows,
        ),
        compiler_params=pltpu.CompilerParams(vmem_limit_bytes=16 * 2**20),
    )(queries, earlier, keys, out_grad)


def completed_kernel(count, *refs):
    own, returned = refs[:2], refs[2:4]
    grads_ref, *sent = refs[4 + count : 5 + 2 * count]
    tokens = own[0].shape[0]
    for half in range(2):
        for block in range(KVH // 2):
            at = slice(block * HD, (block + 1) * HD)
            row = (half * KVH // 2 + block) * tokens
            grads_ref[row : row + tokens, :] = (
                own[half][:, at] + returned[half][:, at].astype(jnp.float32)
            ).astype(jnp.bfloat16)
    for out_ref in sent:
        out_ref[COLUMNS:, :] = grads_ref[...]


def completed(own, returned, pieces):
    count = len(pieces)
    shape = jax.ShapeDtypeStruct((KVH * own[0].shape[0], HD), jnp.bfloat16)
    return pl.pallas_call(
        functools.partial(completed_kernel, count),
        name="complete",
        out_shape=(shape, *(jax.ShapeDtypeStruct(p.shape, p.dtype) for p in pieces)),
        in_specs=[VMEM] * (4 + count),
        out_specs=tuple([VMEM] * (1 + count)),
        input_output_aliases={4 + i: 1 + i for i in range(count)},
        cost_estimate=pl.CostEstimate(flops=5 * 10**8, bytes_accessed=2**20, transcendentals=0),
        compiler_params=pltpu.CompilerParams(vmem_limit_bytes=4 * 2**20),
    )(*own, *returned, *pieces)


def multiply_kernel(places, offs, away, *refs):
    count = 1 + max(max(left, grads) for way in places for left, (grads, _) in way)
    arrays, rest = refs[:count], refs[count:]
    tile = COLUMNS // SIDE
    core = lax.axis_index("c")

    def product(way, at):
        def right(place):
            which, base = place
            tokens = arrays[which].shape[1]
            return jnp.concatenate(
                [
                    arrays[which][base + block * tokens : base + (block + 1) * tokens, :]
                    for block in range(KVH)
                ],
                axis=1,
            )

        total = None
        for i in range(0, SIDE, 2):
            (left_a, grads_a), (left_b, grads_b) = places[way][i], places[way][i + 1]
            left = jnp.concatenate([arrays[left_a][at, :], arrays[left_b][at, :]], axis=1)
            both = jnp.concatenate([right(grads_a), right(grads_b)], axis=0)
            term = jnp.dot(left, both, preferred_element_type=jnp.float32)
            total = term if total is None else total + term
        return total

    def work(way):
        def step(number, carry):
            off = offs[0] + number * (offs[1] - offs[0])
            total = product(way, pl.ds(pl.multiple_of(off * tile, tile), tile))
            at = pl.ds(pl.multiple_of(number * tile, tile), tile)
            if away:
                rest[0][at, :] = total.astype(jnp.bfloat16)
                return carry
            total = (total + rest[0][at, :].astype(jnp.float32)).astype(jnp.bfloat16)
            for which in range(2):

                @pl.when(number == which)
                def _():
                    rest[1 + which][...] = total

            return carry

        lax.fori_loop(0, 2, step, 0)

    for way in range(2):

        @pl.when(core == (1 - way if away else way))
        def _():
            work(way)


def multiplied(offs, ways, got=None):
    arrays, places = [], []
    for pairs in ways:
        way = []
        for columns, grads in pairs:
            found = []
            for array in (columns, grads):
                if array is not None:
                    known = [i for i, other in enumerate(arrays) if other is array]
                    if not known:
                        arrays.append(array)
                    found.append(known[0] if known else len(arrays) - 1)
            way.append((found[0], (found[0], COLUMNS) if grads is None else (found[1], 0)))
        places.append(tuple(way))
    tile = COLUMNS // SIDE
    away = got is None
    shapes = [(len(offs) * tile, WIDTH)] if away else [(tile, WIDTH)] * len(offs)
    operands = arrays if away else arrays + [got]
    return pl.pallas_call(
        functools.partial(multiply_kernel, tuple(places), offs, away),
        name="multiply",
        out_shape=tuple(jax.ShapeDtypeStruct(shape, jnp.bfloat16) for shape in shapes),
        in_specs=[VMEM] * len(operands),
        out_specs=tuple([VMEM] * len(shapes)),
        cost_estimate=pl.CostEstimate(
            flops=2 * len(offs) * tile * SIDE * 128 * WIDTH,
            bytes_accessed=4 * 2**20,
            transcendentals=0,
        ),
        compiler_params=pltpu.CompilerParams(vmem_limit_bytes=16 * 2**20),
    )(*operands)


def halfway_kernel(*refs):
    parts, out_ref = refs[:-1], refs[-1]
    z = lax.axis_index(Z)
    for block in range(Z_SIZE):
        at = slice(block * OWNED, (block + 1) * OWNED)
        total = parts[0][at, :].astype(jnp.float32)
        for part in parts[1:]:
            total += part[at, :].astype(jnp.float32)
        out_ref[(z + block) & (Z_SIZE - 1)] = total.astype(out_ref.dtype)


def halfway(parts):
    return pl.pallas_call(
        halfway_kernel,
        name="halfway",
        out_shape=jax.ShapeDtypeStruct((Z_SIZE, OWNED, WIDTH), jnp.bfloat16),
        in_specs=[VMEM] * len(parts),
        out_specs=VMEM,
        cost_estimate=pl.CostEstimate(flops=5 * 10**8, bytes_accessed=2**20, transcendentals=0),
        compiler_params=pltpu.CompilerParams(vmem_limit_bytes=4 * 2**20),
    )(*parts)


def finish_kernel(parts_ref, out_ref):
    total = parts_ref[0].astype(jnp.float32)
    for part in range(1, Z_SIZE):
        total += parts_ref[part].astype(jnp.float32)
    out_ref[...] = total


def finished(parts):
    return pl.pallas_call(
        finish_kernel,
        name="finish",
        out_shape=jax.ShapeDtypeStruct((OWNED, WIDTH), jnp.float32),
        in_specs=[VMEM],
        out_specs=VMEM,
        cost_estimate=pl.CostEstimate(flops=5 * 10**8, bytes_accessed=2**20, transcendentals=0),
        compiler_params=pltpu.CompilerParams(vmem_limit_bytes=4 * 2**20),
    )(parts)


def ahead(value, axis, steps):
    count = lax.axis_size(axis)
    return lax.ppermute(value, axis, [(i, (i + steps) % count) for i in range(count)])


def crossed(value, steps):
    pairs = []
    for y in range(SIDE):
        for x in range(SIDE):
            pairs.append(((y * SIDE + x) * 2, ((y + steps) % SIDE * SIDE + x) * 2))
            pairs.append(((y * SIDE + x) * 2 + 1, (y * SIDE + (x + steps) % SIDE) * 2 + 1))
    return lax.ppermute(value, ("y", "x", "c"), pairs)


FAR = (("x", 2), ("y", 2))
NEXT = (("x", 1), ("x", 3), ("y", 1), ("y", 3))
HERE = (("x", 0), ("y", 0))


def body(activations, queries, keys, out_grad, layout):
    columns = {}
    earlier = lax.ppermute(keys, "zl", [(0, 1)])
    flipped, *pieces = picked_rows(
        FAR,
        pltpu.with_memory_space_constraint(layout, pltpu.HBM),
        pltpu.with_memory_space_constraint(activations, pltpu.HBM),
        True,
    )
    for route, piece in zip(FAR, pieces):
        columns[route] = ahead(piece, *route)
    groups = KVH // 2
    own, returned = [], []
    for half in range(2):
        early, mine = attended(half * groups, groups, queries, earlier, keys, out_grad)
        own.append(mine)
        returned.append(lax.ppermute(early, "zl", [(1, 0)]))
    pieces = picked_rows(NEXT, layout, flipped, False, WIDTH)
    value_grad, *pieces = completed(own, returned, pieces)
    pairs = {}
    for route, piece in zip(NEXT, pieces):
        pairs[route] = (ahead(piece, *route), None)
    for route in FAR:
        pairs[route] = (columns[route], ahead(value_grad, *route))
    pieces = picked_rows(HERE, layout, flipped, False)
    for route, piece in zip(HERE, pieces):
        pairs[route] = (piece, value_grad)
    ways = [[pairs[way, steps] for steps in range(SIDE)] for way in WAYS]
    halves = ((1, 3), (2, 0))
    got = []
    for offs in halves:
        (away,) = multiplied(offs, ways)
        got.append(ahead(away, "c", 1))
    parts = []
    for half, offs in enumerate(halves):
        terms = multiplied(offs, ways, got[half])
        for steps, term in zip(offs, terms):
            parts.append(crossed(term, steps) if steps else term)
    terms = halfway(parts)
    terms = lax.all_to_all(terms, Z, 0, 0, tiled=True)
    return finished(terms)


def solution(mesh):
    finer = Mesh(mesh.devices.reshape(4, 4, 4, 2, mesh.shape["seq"]), AXES)
    placed = (P(AXES, None), P(AXES, None), P(AXES, None), P(AXES, None), P())
    return jax.shard_map(
        body, mesh=finer, in_specs=placed, out_specs=P(AXES, None), check_vma=False
    )
```

```python
import functools

import jax
import jax.numpy as jnp
from jax import lax
from jax.experimental import pallas as pl
from jax.experimental.pallas import tpu as pltpu
from jax.sharding import Mesh
from jax.sharding import PartitionSpec as P


H = 64
KVH = 8
HD = 128
WIDTH = KVH * HD
PER = H // KVH
AXES = ("y", "zh", "x", "c", "zl")
Z = ("zh", "zl")
SIDE, Z_SIZE = 4, 8
OWNED = 32
COLUMNS = SIDE * Z_SIZE * OWNED
WAYS = ("x", "y")
SCALE = 1.4426950408889634 / float(HD) ** 0.5
SMEM = pl.BlockSpec(memory_space=pltpu.SMEM)
VMEM = pl.BlockSpec(memory_space=pltpu.VMEM)


def flip(acts_ref, flipped, landed, arrivals):
    width = acts_ref.shape[1]
    count = arrivals.shape[0]
    share = width // count

    def arriving(part):
        at = pl.ds(pl.multiple_of(part * share, share), share)
        return pltpu.make_async_copy(acts_ref.at[:, at], landed.at[:, at], arrivals.at[part])

    for part in range(count):
        arriving(part).start()

    def step(part, carry):
        arriving(part).wait()
        for tile in range(share // 128):
            at = pl.ds(pl.multiple_of(part * share + tile * 128, 128), 128)
            flipped[at, :] = landed[:, at].astype(jnp.float32).T
        return carry

    lax.fori_loop(0, count, step, 0)


def pick(routes, layout_ref, flipped, picked, outs):
    y, z, x = (lax.axis_index(axis) for axis in ("y", Z, "x"))
    for (axis, steps), out_ref in zip(routes, outs):

        def step(tile, carry):
            off = tile >> 1
            x_steps, y_steps = (steps, off) if axis == "x" else (off, steps)
            to_x, to_y = (x + x_steps) & (SIDE - 1), (y + y_steps) & (SIDE - 1)
            for block in range(Z_SIZE // 2):
                to_z = (z + (tile & 1) * (Z_SIZE // 2) + block) & (Z_SIZE - 1)
                owner = (((to_y * 4 + (to_z >> 1)) * 4 + to_x) * 2 + WAYS.index(axis)) * 2 + (to_z & 1)
                for row in range(OWNED):
                    source = layout_ref[owner * OWNED + row]
                    at = block * OWNED + row
                    picked[at : at + 1, :] = flipped[pl.ds(source, 1), :]
            rows = Z_SIZE // 2 * OWNED
            out_ref[pl.ds(pl.multiple_of(tile * rows, rows), rows), :] = picked[...].astype(
                jnp.bfloat16
            )
            return carry

        lax.fori_loop(0, 2 * SIDE, step, 0)


def first_pick_kernel(routes, layout_ref, acts_ref, flipped, *refs):
    outs = refs[: len(routes)]
    picked, landed, arrivals, rows_ref, rows_arrival = refs[len(routes) :]
    rows_copy = pltpu.make_async_copy(layout_ref, rows_ref, rows_arrival)
    rows_copy.start()
    flip(acts_ref, flipped, landed, arrivals)
    rows_copy.wait()
    pick(routes, rows_ref, flipped, picked, outs)


def later_pick_kernel(routes, layout_ref, flipped, *refs):
    pick(routes, layout_ref, flipped, refs[-1], refs[:-1])


def picked_rows(routes, layout, source, first, spare=0):
    tokens = 128
    width = layout.shape[0]
    piece = jax.ShapeDtypeStruct((COLUMNS + spare, tokens), jnp.bfloat16)
    shapes = [piece] * len(routes)
    scratch = [pltpu.VMEM((Z_SIZE // 2 * OWNED, tokens), jnp.float32)]
    if first:
        shapes = [jax.ShapeDtypeStruct((width, tokens), jnp.float32)] + shapes
        scratch += [
            pltpu.VMEM((tokens, width), jnp.bfloat16),
            pltpu.SemaphoreType.DMA((8,)),
            pltpu.SMEM((width,), jnp.int32),
            pltpu.SemaphoreType.DMA,
        ]
    far = pl.BlockSpec(memory_space=pltpu.HBM)
    return pl.pallas_call(
        functools.partial(first_pick_kernel if first else later_pick_kernel, routes),
        name="pick",
        out_shape=tuple(shapes),
        in_specs=[far, far] if first else [SMEM, VMEM],
        out_specs=tuple([VMEM] * len(shapes)),
        scratch_shapes=scratch,
        cost_estimate=pl.CostEstimate(
            flops=10**9 * len(routes), bytes_accessed=4 * 2**20, transcendentals=0
        ),
        compiler_params=pltpu.CompilerParams(vmem_limit_bytes=16 * 2**20),
    )(layout, source)


def attend_kernel(
    first, groups, queries_ref, earlier_ref, keys_ref, grads_ref, early_ref, own_ref
):
    rows = queries_ref.shape[0]
    second = lax.axis_index("zl") > 0
    shape = (rows, rows)
    causal = lax.broadcasted_iota(jnp.int32, shape, 0) <= lax.broadcasted_iota(jnp.int32, shape, 1)

    def group(number, carry):
        head = pl.ds(pl.multiple_of((number + first) * HD, HD), HD)
        both = jnp.concatenate([earlier_ref[:, head], keys_ref[:, head]], axis=0)
        total = jnp.zeros((2 * rows, HD), jnp.float32)
        for query_head in range(PER):
            at = pl.ds(pl.multiple_of(((number + first) * PER + query_head) * HD, HD), HD)
            scores = lax.dot_general(
                both, queries_ref[:, at], (((1,), (1,)), ((), ())), preferred_element_type=jnp.float32
            )
            before = jnp.where(second, scores[:rows], -1e30)
            last = jnp.where(causal, scores[rows:], -1e30)
            top = jnp.maximum(
                jnp.max(before, axis=0, keepdims=True), jnp.max(last, axis=0, keepdims=True)
            )
            before = jnp.exp2((before - top) * SCALE)
            last = jnp.exp2((last - top) * SCALE)
            share = 1.0 / (
                jnp.sum(before, axis=0, keepdims=True) + jnp.sum(last, axis=0, keepdims=True)
            )
            weights = jnp.concatenate(
                [(before * share).astype(jnp.bfloat16), (last * share).astype(jnp.bfloat16)], axis=0
            )
            total += jnp.dot(weights, grads_ref[:, at], preferred_element_type=jnp.float32)
        out = pl.ds(pl.multiple_of(number * HD, HD), HD)
        early_ref[:, out] = total[:rows].astype(early_ref.dtype)
        own_ref[:, out] = total[rows:]
        return carry

    lax.fori_loop(0, groups, group, 0)


def attended(first, groups, queries, earlier, keys, out_grad):
    rows = queries.shape[0]
    return pl.pallas_call(
        functools.partial(attend_kernel, first, groups),
        name="attend",
        out_shape=(
            jax.ShapeDtypeStruct((rows, groups * HD), jnp.bfloat16),
            jax.ShapeDtypeStruct((rows, groups * HD), jnp.float32),
        ),
        in_specs=[VMEM, VMEM, VMEM, VMEM],
        out_specs=(VMEM, VMEM),
        cost_estimate=pl.CostEstimate(
            flops=4 * groups * PER * rows * 2 * rows * HD,
            bytes_accessed=3 * 2**20,
            transcendentals=groups * PER * rows * 2 * rows,
        ),
        compiler_params=pltpu.CompilerParams(vmem_limit_bytes=16 * 2**20),
    )(queries, earlier, keys, out_grad)


def completed_kernel(count, *refs):
    own, returned = refs[:2], refs[2:4]
    grads_ref, *sent = refs[4 + count : 5 + 2 * count]
    tokens = own[0].shape[0]
    for half in range(2):
        for block in range(KVH // 2):
            at = slice(block * HD, (block + 1) * HD)
            row = (half * KVH // 2 + block) * tokens
            grads_ref[row : row + tokens, :] = (
                own[half][:, at] + returned[half][:, at].astype(jnp.float32)
            ).astype(jnp.bfloat16)
    for out_ref in sent:
        out_ref[COLUMNS:, :] = grads_ref[...]


def completed(own, returned, pieces):
    count = len(pieces)
    shape = jax.ShapeDtypeStruct((KVH * own[0].shape[0], HD), jnp.bfloat16)
    return pl.pallas_call(
        functools.partial(completed_kernel, count),
        name="complete",
        out_shape=(shape, *(jax.ShapeDtypeStruct(p.shape, p.dtype) for p in pieces)),
        in_specs=[VMEM] * (4 + count),
        out_specs=tuple([VMEM] * (1 + count)),
        input_output_aliases={4 + i: 1 + i for i in range(count)},
        cost_estimate=pl.CostEstimate(flops=5 * 10**8, bytes_accessed=2**20, transcendentals=0),
        compiler_params=pltpu.CompilerParams(vmem_limit_bytes=4 * 2**20),
    )(*own, *returned, *pieces)


def multiply_kernel(places, offs, away, *refs):
    count = 1 + max(max(left, grads) for way in places for left, (grads, _) in way)
    arrays, rest = refs[:count], refs[count:]
    tile = COLUMNS // SIDE
    core = lax.axis_index("c")

    def product(way, at):
        def right(place):
            which, base = place
            tokens = arrays[which].shape[1]
            return jnp.concatenate(
                [
                    arrays[which][base + block * tokens : base + (block + 1) * tokens, :]
                    for block in range(KVH)
                ],
                axis=1,
            )

        total = None
        for i in range(0, SIDE, 2):
            (left_a, grads_a), (left_b, grads_b) = places[way][i], places[way][i + 1]
            left = jnp.concatenate([arrays[left_a][at, :], arrays[left_b][at, :]], axis=1)
            both = jnp.concatenate([right(grads_a), right(grads_b)], axis=0)
            term = jnp.dot(left, both, preferred_element_type=jnp.float32)
            total = term if total is None else total + term
        return total

    def work(way):
        def step(number, carry):
            off = (offs[0] + number) & (SIDE - 1)
            total = product(way, pl.ds(pl.multiple_of(off * tile, tile), tile))
            at = pl.ds(pl.multiple_of(number * tile, tile), tile)
            if away:
                rest[0][at, :] = total.astype(jnp.bfloat16)
                return carry
            total = (total + rest[0][at, :].astype(jnp.float32)).astype(jnp.bfloat16)
            for which in range(len(offs)):

                @pl.when(number == which)
                def _():
                    rest[1 + which][...] = total

            return carry

        lax.fori_loop(0, len(offs), step, 0)

    for way in range(2):

        @pl.when(core == (1 - way if away else way))
        def _():
            work(way)


def multiplied(offs, ways, got=None):
    arrays, places = [], []
    for pairs in ways:
        way = []
        for columns, grads in pairs:
            found = []
            for array in (columns, grads):
                if array is not None:
                    known = [i for i, other in enumerate(arrays) if other is array]
                    if not known:
                        arrays.append(array)
                    found.append(known[0] if known else len(arrays) - 1)
            way.append((found[0], (found[0], COLUMNS) if grads is None else (found[1], 0)))
        places.append(tuple(way))
    tile = COLUMNS // SIDE
    away = got is None
    shapes = [(len(offs) * tile, WIDTH)] if away else [(tile, WIDTH)] * len(offs)
    operands = arrays if away else arrays + [got]
    return pl.pallas_call(
        functools.partial(multiply_kernel, tuple(places), offs, away),
        name="multiply",
        out_shape=tuple(jax.ShapeDtypeStruct(shape, jnp.bfloat16) for shape in shapes),
        in_specs=[VMEM] * len(operands),
        out_specs=tuple([VMEM] * len(shapes)),
        cost_estimate=pl.CostEstimate(
            flops=2 * len(offs) * tile * SIDE * 128 * WIDTH,
            bytes_accessed=4 * 2**20,
            transcendentals=0,
        ),
        compiler_params=pltpu.CompilerParams(vmem_limit_bytes=16 * 2**20),
    )(*operands)


def halfway_kernel(*refs):
    parts, out_ref = refs[:-1], refs[-1]
    z = lax.axis_index(Z)
    for block in range(Z_SIZE):
        at = slice(block * OWNED, (block + 1) * OWNED)
        total = parts[0][at, :].astype(jnp.float32)
        for part in parts[1:]:
            total += part[at, :].astype(jnp.float32)
        out_ref[(z + block) & (Z_SIZE - 1)] = total.astype(out_ref.dtype)


def halfway(parts):
    return pl.pallas_call(
        halfway_kernel,
        name="halfway",
        out_shape=jax.ShapeDtypeStruct((Z_SIZE, OWNED, WIDTH), jnp.bfloat16),
        in_specs=[VMEM] * len(parts),
        out_specs=VMEM,
        cost_estimate=pl.CostEstimate(flops=5 * 10**8, bytes_accessed=2**20, transcendentals=0),
        compiler_params=pltpu.CompilerParams(vmem_limit_bytes=4 * 2**20),
    )(*parts)


def finish_kernel(parts_ref, out_ref):
    total = parts_ref[0].astype(jnp.float32)
    for part in range(1, Z_SIZE):
        total += parts_ref[part].astype(jnp.float32)
    out_ref[...] = total


def finished(parts):
    return pl.pallas_call(
        finish_kernel,
        name="finish",
        out_shape=jax.ShapeDtypeStruct((OWNED, WIDTH), jnp.float32),
        in_specs=[VMEM],
        out_specs=VMEM,
        cost_estimate=pl.CostEstimate(flops=5 * 10**8, bytes_accessed=2**20, transcendentals=0),
        compiler_params=pltpu.CompilerParams(vmem_limit_bytes=4 * 2**20),
    )(parts)


def ahead(value, axis, steps):
    count = lax.axis_size(axis)
    return lax.ppermute(value, axis, [(i, (i + steps) % count) for i in range(count)])


def crossed(value, steps):
    pairs = []
    for y in range(SIDE):
        for x in range(SIDE):
            pairs.append(((y * SIDE + x) * 2, ((y + steps) % SIDE * SIDE + x) * 2))
            pairs.append(((y * SIDE + x) * 2 + 1, (y * SIDE + (x + steps) % SIDE) * 2 + 1))
    return lax.ppermute(value, ("y", "x", "c"), pairs)


FAR = (("x", 2), ("y", 2))
NEXT = (("x", 1), ("x", 3), ("y", 1), ("y", 3))
HERE = (("x", 0), ("y", 0))


def body(activations, queries, keys, out_grad, layout):
    columns = {}
    earlier = lax.ppermute(keys, "zl", [(0, 1)])
    flipped, *pieces = picked_rows(
        FAR,
        pltpu.with_memory_space_constraint(layout, pltpu.HBM),
        pltpu.with_memory_space_constraint(activations, pltpu.HBM),
        True,
    )
    for route, piece in zip(FAR, pieces):
        columns[route] = ahead(piece, *route)
    groups = KVH // 2
    own, returned = [], []
    for half in range(2):
        early, mine = attended(half * groups, groups, queries, earlier, keys, out_grad)
        own.append(mine)
        returned.append(lax.ppermute(early, "zl", [(1, 0)]))
    pieces = picked_rows(NEXT, layout, flipped, False, WIDTH)
    value_grad, *pieces = completed(own, returned, pieces)
    pairs = {}
    for route, piece in zip(NEXT, pieces):
        pairs[route] = (ahead(piece, *route), None)
    for route in FAR:
        pairs[route] = (columns[route], ahead(value_grad, *route))
    pieces = picked_rows(HERE, layout, flipped, False)
    for route, piece in zip(HERE, pieces):
        pairs[route] = (piece, value_grad)
    ways = [[pairs[way, steps] for steps in range(SIDE)] for way in WAYS]
    halves = ((2,), (3, 0, 1))
    got = []
    for offs in halves:
        (away,) = multiplied(offs, ways)
        got.append(ahead(away, "c", 1))
    parts = []
    for half, offs in enumerate(halves):
        terms = multiplied(offs, ways, got[half])
        for steps, term in zip(offs, terms):
            parts.append(crossed(term, steps) if steps else term)
    terms = halfway(parts)
    terms = lax.all_to_all(terms, Z, 0, 0, tiled=True)
    return finished(terms)


def solution(mesh):
    finer = Mesh(mesh.devices.reshape(4, 4, 4, 2, mesh.shape["seq"]), AXES)
    placed = (P(AXES, None), P(AXES, None), P(AXES, None), P(AXES, None), P())
    return jax.shard_map(
        body, mesh=finer, in_specs=placed, out_specs=P(AXES, None), check_vma=False
    )
```
